32 devices in a mesh: horiz: 8 (over y, x, core), lev: 4 (over z).
Axes of the slice: x: 2, y: 2, z: 4, core: 2. Of those that a mesh axis runs over, the one named last changes fastest.
Arguments:
- source_state: bfloat16 [5, 68, 32768], P(None, 'lev', 'horiz'), may hold values from -6 to 6
- intersection: int32 [40], P('horiz'), may hold values from 0 to 7, as said below
- index_map: int32 [40, 512], P('horiz'), may hold values from 0 to 4095
- blocks: bfloat16 [40, 512, 2048], P('horiz'), may hold values from -0.125 to 0.125
- bracket: int32 [127, 16384], P(None, ('horiz', 'lev')), may hold values from 0 to 66
- fraction: float32 [127, 16384], P(None, ('horiz', 'lev')), may hold values from 0 to 1
Outputs:
- target_state: bfloat16 [5, 127, 16384], P(None, None, ('horiz', 'lev'))
The draws below stay inside these ranges and needn't reach their ends.
Inputs may be any that keep to these rules, and one draw needn't show every extreme that they name: For every target group g, intersection[g * 5] to intersection[g * 5 + 4] are the groups g - 2 to g + 2 modulo 8, each once, in some order.
All inputs are finite; a program needn't handle non-finite values.
Results may differ from the reference program's by a relative error of at most 0.0049.
Values may be sent and summed in bfloat16 or wider, within the bound.
A program may use at most 64 MiB of HBM per device.

```python
import jax
import jax.numpy as jnp
from jax import lax

F = 5
LEVELS_OUT = 127
R = 2
SRC_DEV = 4096
P_SIZE = 512
TGT_DEV = 2048
K = 5
GROUPS = 8
LEVELS_IN = 68
SRC_CELLS = 32768
TGT_CELLS = 16384
BLOCKS = 40


def draw_intersection(key, part):
    subkeys = jax.random.split(key, GROUPS)
    orders = jax.vmap(lambda subkey: jax.random.permutation(subkey, K))(subkeys)
    group_ids = jnp.arange(GROUPS, dtype=jnp.int32)[:, None]
    return ((group_ids + orders.astype(jnp.int32) - R) % GROUPS).reshape(-1).astype(jnp.int32)


def plant(drawn, key, least, high):
    extent = drawn.shape
    spot = [jax.random.randint(jax.random.fold_in(key, axis), (), 0, extent[axis]) for axis in range(len(extent))]
    drawn = drawn.at[tuple(spot)].set(least)
    longest = extent.index(max(extent))
    spot[longest] = (spot[longest] + 1) % extent[longest]
    return drawn.at[tuple(spot)].set(high)


def block_levels(key, extent, shards, smallest, top_value):
    def one(dim, parts):
        heights = jax.random.uniform(jax.random.fold_in(jax.random.fold_in(key, 6), dim), (parts,), jnp.float32, smallest / len(shards), top_value / len(shards))
        return jnp.repeat(jnp.exp(heights), extent[dim] // parts).reshape((-1,) + (1,) * (len(extent) - dim - 1))

    loudness = one(*shards[0])
    for cut in shards[1:]:
        loudness = loudness * one(*cut)
    return loudness


def scatter_about(key, dims, deviation, limit, pieces=(), held_as=jnp.bfloat16):
    array = jax.random.normal(key, dims, jnp.float32) * deviation
    if len(pieces) > 0:
        array = block_levels(key, dims, pieces, -0.22, 0.18) * array
    return jnp.clip(array, min=-limit, max=limit).astype(held_as)


def setup_inputs(seed: int = 0) -> dict:
    key_of = jax.random.split(jax.random.key(seed), 7)
    source_state = scatter_about(key_of[0], (F, LEVELS_IN, SRC_CELLS), 1.0, 6.0, ((1, 4), (2, 8)))
    intersection = draw_intersection(jax.random.fold_in(key_of[6], 71), 0)
    index_map = plant(jax.random.randint(key_of[2], (BLOCKS, P_SIZE), 0, SRC_DEV), jax.random.fold_in(key_of[2], 1), 0, SRC_DEV - 1).astype(jnp.int32)
    blocks = scatter_about(key_of[3], (BLOCKS, P_SIZE, TGT_DEV), (K * P_SIZE) ** -0.5, 0.125, ((0, 8),))
    bracket = plant(jax.random.randint(key_of[4], (LEVELS_OUT, TGT_CELLS), 0, LEVELS_IN - 1), jax.random.fold_in(key_of[4], 1), 0, (LEVELS_IN - 1) - 1).astype(jnp.int32)
    fraction = jnp.clip(1.0 * jax.random.uniform(key_of[5], (LEVELS_OUT, TGT_CELLS), jnp.float32) ** block_levels(key_of[5], (LEVELS_OUT, TGT_CELLS), ((1, 32),), -0.2, 0.2), 0.0, 1.0)
    return {"source_state": source_state, "intersection": intersection, "index_map": index_map, "blocks": blocks, "bracket": bracket, "fraction": fraction}


def reference(source_state, intersection, index_map, blocks, bracket, fraction):
    group_count = intersection.shape[0] // K
    fields_levels = F * LEVELS_IN
    source_tiles = jnp.transpose(source_state.reshape(fields_levels, group_count, SRC_DEV), (1, 0, 2))

    def remap_group(group_id):
        total_sum = jnp.zeros((fields_levels, TGT_DEV), jnp.float32)
        for block_slot in range(K):
            block_row = group_id * K + block_slot
            source_tile = source_tiles[intersection[block_row]]
            chosen = jnp.take(source_tile, index_map[block_row], axis=1).astype(jnp.float32)
            weights = blocks[block_row].astype(jnp.float32)
            total_sum = total_sum + jnp.dot(chosen, weights, preferred_element_type=jnp.float32)
        return total_sum.astype(jnp.bfloat16)

    remapped = lax.map(remap_group, jnp.arange(group_count, dtype=jnp.int32))
    horizontal = jnp.transpose(remapped, (1, 0, 2)).reshape(F, LEVELS_IN, group_count * TGT_DEV)
    widened = horizontal.astype(jnp.float32)
    below_level = jnp.take_along_axis(widened, bracket[None], axis=1)
    above_level = jnp.take_along_axis(widened, bracket[None] + 1, axis=1)
    upper_share = fraction[None]
    return ((1.0 - upper_share) * below_level + upper_share * above_level).astype(jnp.bfloat16)
```

```python
import functools

import jax
import jax.numpy as jnp
from jax import lax
from jax.experimental import pallas as pl
from jax.experimental.pallas import tpu as pltpu
from jax.sharding import PartitionSpec as P

MESH = pl.DeviceIdType.MESH
HIGH = 256


def round_up(value, step):
    return (value + step - 1) // step * step


def remap_kernel(
    groups, levs, depth,
    inter_ref, index_ref, source_hbm, blocks_hbm, out_ref,
    tile, stack32, stack, weights, request, wanted, chosen, arrived, total, slab,
    tile_sem, weight_sem, req_send, req_recv, val_send, val_recv, lev_send, lev_recv,
):
    fields, slab_levels, cells = tile.shape
    rows = stack.shape[0]
    count = 2 * depth + 1
    me = lax.axis_index("horiz")
    my_lev = lax.axis_index("lev")
    columns = out_ref.shape[2]

    barrier = pltpu.get_barrier_semaphore()
    offsets = [o for o in range(-depth, depth + 1) if o != 0]
    for offset in offsets:
        pl.semaphore_signal(
            barrier, inc=1, device_id={"horiz": lax.rem(me + offset + groups, groups)}, device_id_type=MESH
        )
    for hop in range(1, levs):
        pl.semaphore_signal(
            barrier, inc=1, device_id={"lev": lax.rem(my_lev + hop, levs)}, device_id_type=MESH
        )

    tile_copy = pltpu.make_async_copy(source_hbm, tile, tile_sem)
    tile_copy.start()
    weight_copies = []
    for part in range(levs):
        copy = pltpu.make_async_copy(
            blocks_hbm.at[:, :, pl.ds(part * columns, columns)], weights.at[:, part], weight_sem.at[part]
        )
        copy.start()
        weight_copies.append(copy)

    slots = []
    for place in range(count):
        group = lax.rem(me + place - depth + groups, groups)
        cells_wanted = jnp.zeros((1, index_ref.shape[1]), jnp.int32)
        slot = jnp.int32(0)
        for k in range(count):
            hit = (inter_ref[k] == group).astype(jnp.int32)
            cells_wanted = cells_wanted + index_ref[k : k + 1, :] * hit
            slot = jnp.where(inter_ref[k] == group, jnp.int32(k), slot)
        slots.append(slot)
        if place == depth:
            wanted[place] = cells_wanted
        else:
            request[place] = cells_wanted

    tile_copy.wait()
    for field in range(fields):
        stack32[pl.ds(field * slab_levels, slab_levels), :] = tile[field].astype(jnp.float32)
    spare = rows - fields * slab_levels
    if spare:
        stack32[pl.ds(fields * slab_levels, spare), :] = jnp.zeros((spare, cells), jnp.float32)
    stack[...] = stack32[...].astype(jnp.bfloat16)

    pl.semaphore_wait(barrier, len(offsets) + levs - 1)

    def request_copy(place):
        return pltpu.make_async_remote_copy(
            src_ref=request.at[place],
            dst_ref=wanted.at[2 * depth - place],
            send_sem=req_send.at[place],
            recv_sem=req_recv.at[2 * depth - place],
            device_id={"horiz": lax.rem(me + place - depth + groups, groups)},
            device_id_type=MESH,
        )

    def value_copy(place):
        return pltpu.make_async_remote_copy(
            src_ref=chosen.at[place],
            dst_ref=arrived.at[2 * depth - place],
            send_sem=val_send.at[place],
            recv_sem=val_recv.at[2 * depth - place],
            device_id={"horiz": lax.rem(me + place - depth + groups, groups)},
            device_id_type=MESH,
        )

    for reach in range(depth, 0, -1):
        request_copy(depth - reach).start()
        request_copy(depth + reach).start()

    ids = lax.broadcasted_iota(jnp.int32, (HIGH, 1), 0).astype(jnp.float32).astype(jnp.bfloat16)

    def select(place):
        cell = wanted[place]
        high = cell // HIGH
        low = (cell - high * HIGH).astype(jnp.float32)
        values = jnp.zeros((rows, cell.shape[1]), jnp.float32)
        for chunk in range(cells // HIGH):
            here = jnp.where(high == chunk, low, -1.0).astype(jnp.bfloat16)
            picker = jnp.where(ids == here, jnp.bfloat16(1), jnp.bfloat16(0))
            values += jnp.dot(
                stack[:, chunk * HIGH : (chunk + 1) * HIGH], picker, preferred_element_type=jnp.float32
            )
        return values.astype(jnp.bfloat16)

    arrived[depth] = select(depth)

    def serve(step, carry):
        reach = depth - step // 2
        place = depth + reach * (1 - 2 * (step % 2))
        request_copy(2 * depth - place).wait_recv()
        chosen[place] = select(place)
        value_copy(place).start()
        return carry

    lax.fori_loop(0, 2 * depth, serve, 0)

    for copy in weight_copies:
        copy.wait()
    order = [depth]
    for reach in range(depth, 0, -1):
        order += [depth - reach, depth + reach]
    for number, place in enumerate(order):
        if number:
            value_copy(2 * depth - place).wait_recv()
        values = arrived[place]
        for hop in list(range(1, levs)) + [0]:
            part = lax.rem(my_lev + hop, levs)
            term = jnp.dot(values, weights[slots[place], part], preferred_element_type=jnp.float32)
            if number == 0:
                total[part] = term
            elif number < count - 1:
                total[part] += term
            else:
                done = (total[part] + term).astype(jnp.bfloat16)
                if hop == 0:
                    out_ref[my_lev] = done
                else:
                    slab[hop] = done
                    lev_copy(hop, part, my_lev, slab, out_ref, lev_send, lev_recv).start()
    for hop in range(1, levs):
        lev_copy(hop, lax.rem(my_lev + hop, levs), my_lev, slab, out_ref, lev_send, lev_recv).wait()
    for offset in offsets:
        request_copy(depth + offset).wait_send()
        value_copy(depth + offset).wait_send()


def lev_copy(hop, part, my_lev, slab, out_ref, lev_send, lev_recv):
    return pltpu.make_async_remote_copy(
        src_ref=slab.at[hop],
        dst_ref=out_ref.at[my_lev],
        send_sem=lev_send.at[hop],
        recv_sem=lev_recv.at[hop],
        device_id={"lev": part},
        device_id_type=MESH,
    )


def rows_at(table, index):
    numbers = lax.GatherDimensionNumbers(
        offset_dims=(),
        collapsed_slice_dims=(0,),
        start_index_map=(0,),
        operand_batching_dims=(1,),
        start_indices_batching_dims=(1,),
    )
    return lax.gather(
        table, index[..., None], numbers, slice_sizes=(1, 1), mode=lax.GatherScatterMode.PROMISE_IN_BOUNDS
    )


def levels_kernel(slab_levels, slabs_ref, bracket_ref, fraction_ref, out_ref, raw, table):
    levs = slabs_ref.shape[0]
    fields, levels_out, lanes = out_ref.shape
    total = levs * slab_levels
    raw[...] = slabs_ref[...].astype(jnp.float32)
    for field in range(fields):
        for lev in range(levs):
            table[field, pl.ds(lev * slab_levels, slab_levels), :] = raw[
                lev, pl.ds(field * slab_levels, slab_levels), :
            ]
        table[field, pl.ds(total, table.shape[1] - total), :] = jnp.zeros(
            (table.shape[1] - total, lanes), jnp.float32
        )
    step = 16
    for start in range(0, levels_out, step):
        size = min(step, levels_out - start)
        bracket = bracket_ref[start : start + size, :]
        upper = fraction_ref[start : start + size, :]
        if size < step:
            bracket = jnp.concatenate([bracket, jnp.zeros((step - size, lanes), jnp.int32)], axis=0)
            upper = jnp.concatenate([upper, jnp.zeros((step - size, lanes), jnp.float32)], axis=0)
        halves = [bracket[i : i + 8] for i in range(0, step, 8)]
        high = [half >> 3 for half in halves]
        low = [half & 7 for half in halves]
        below = [[jnp.zeros((8, lanes), jnp.float32) for _ in halves] for _ in range(fields)]
        above = [[jnp.zeros((8, lanes), jnp.float32) for _ in halves] for _ in range(fields)]
        for group in range((total - 2) // 8 + 1):
            masks = [h == group for h in high]
            for field in range(fields):
                here = table[field, pl.ds(group * 8, 8), :]
                over = table[field, pl.ds(group * 8 + 1, 8), :]
                for i, mask in enumerate(masks):
                    below[field][i] = jnp.where(mask, rows_at(here, low[i]), below[field][i])
                    above[field][i] = jnp.where(mask, rows_at(over, low[i]), above[field][i])
        for field in range(fields):
            mixed = (1.0 - upper) * jnp.concatenate(below[field], axis=0) + upper * jnp.concatenate(
                above[field], axis=0
            )
            out_ref[field, start : start + size, :] = mixed[:size].astype(jnp.bfloat16)


def local(levs, groups, source_state, intersection, index_map, blocks, bracket, fraction):
    fields, slab_levels, cells = source_state.shape
    count, wide, targets = blocks.shape
    depth = (count - 1) // 2
    rows = round_up(fields * slab_levels, 8)
    columns = targets // levs
    slabs = pl.pallas_call(
        functools.partial(remap_kernel, groups, levs, depth),
        name="remap",
        out_shape=jax.ShapeDtypeStruct((levs, rows, columns), jnp.bfloat16),
        in_specs=[
            pl.BlockSpec(memory_space=pltpu.SMEM),
            pl.BlockSpec(memory_space=pltpu.VMEM),
            pl.BlockSpec(memory_space=pl.ANY),
            pl.BlockSpec(memory_space=pl.ANY),
        ],
        out_specs=pl.BlockSpec(memory_space=pltpu.VMEM),
        scratch_shapes=[
            pltpu.VMEM((fields, slab_levels, cells), jnp.bfloat16),
            pltpu.VMEM((rows, cells), jnp.float32),
            pltpu.VMEM((rows, cells), jnp.bfloat16),
            pltpu.VMEM((count, levs, wide, columns), jnp.bfloat16),
            pltpu.VMEM((count, 1, wide), jnp.int32),
            pltpu.VMEM((count, 1, wide), jnp.int32),
            pltpu.VMEM((count, rows, wide), jnp.bfloat16),
            pltpu.VMEM((count, rows, wide), jnp.bfloat16),
            pltpu.VMEM((levs, rows, columns), jnp.float32),
            pltpu.VMEM((levs, rows, columns), jnp.bfloat16),
            pltpu.SemaphoreType.DMA,
            pltpu.SemaphoreType.DMA((levs,)),
            pltpu.SemaphoreType.DMA((count,)),
            pltpu.SemaphoreType.DMA((count,)),
            pltpu.SemaphoreType.DMA((count,)),
            pltpu.SemaphoreType.DMA((count,)),
            pltpu.SemaphoreType.DMA((levs,)),
            pltpu.SemaphoreType.DMA((levs,)),
        ],
        compiler_params=pltpu.CompilerParams(
            collective_id=0, has_side_effects=True, vmem_limit_bytes=48 * 1024 * 1024
        ),
    )(intersection, index_map, source_state, blocks)
    levels_out, held = bracket.shape
    lanes = 128
    return pl.pallas_call(
        functools.partial(levels_kernel, slab_levels),
        name="levels",
        grid=(held // lanes,),
        out_shape=jax.ShapeDtypeStruct((fields, levels_out, held), jnp.bfloat16),
        in_specs=[
            pl.BlockSpec((levs, rows, lanes), lambda i: (0, 0, i)),
            pl.BlockSpec((levels_out, lanes), lambda i: (0, i)),
            pl.BlockSpec((levels_out, lanes), lambda i: (0, i)),
        ],
        out_specs=pl.BlockSpec((fields, levels_out, lanes), lambda i: (0, 0, i)),
        scratch_shapes=[
            pltpu.VMEM((levs, rows, lanes), jnp.float32),
            pltpu.VMEM((fields, round_up(levs * slab_levels, 8) + 8, lanes), jnp.float32),
        ],
    )(slabs, bracket, fraction)


def solution(mesh):
    in_specs = (
        P(None, "lev", "horiz"),
        P("horiz"),
        P("horiz", None),
        P("horiz", None, None),
        P(None, ("horiz", "lev")),
        P(None, ("horiz", "lev")),
    )
    out_specs = P(None, None, ("horiz", "lev"))
    body = functools.partial(local, mesh.shape["lev"], mesh.shape["horiz"])
    return jax.shard_map(body, mesh=mesh, in_specs=in_specs, out_specs=out_specs, check_vma=False)
```

```python
import functools

import jax
import jax.numpy as jnp
from jax import lax
from jax.experimental import pallas as pl
from jax.experimental.pallas import tpu as pltpu
from jax.sharding import PartitionSpec as P

MESH = pl.DeviceIdType.MESH
HIGH = 256


def round_up(value, step):
    return (value + step - 1) // step * step


def remap_kernel(
    groups, levs, depth,
    inter_hbm, index_hbm, source_hbm, blocks_hbm, out_ref,
    inter_ref, index_ref, tile, stack32, stack, weights, request, wanted, chosen, arrived, total, slab,
    inter_sem, index_sem, tile_sem, weight_sem, req_send, req_recv, val_send, val_recv, lev_send, lev_recv,
):
    fields, slab_levels, cells = tile.shape
    rows = stack.shape[0]
    count = 2 * depth + 1
    me = lax.axis_index("horiz")
    my_lev = lax.axis_index("lev")
    columns = out_ref.shape[2]

    barrier = pltpu.get_barrier_semaphore()
    offsets = [o for o in range(-depth, depth + 1) if o != 0]
    for offset in offsets:
        pl.semaphore_signal(
            barrier, inc=1, device_id={"horiz": lax.rem(me + offset + groups, groups)}, device_id_type=MESH
        )
    for hop in range(1, levs):
        pl.semaphore_signal(
            barrier, inc=1, device_id={"lev": lax.rem(my_lev + hop, levs)}, device_id_type=MESH
        )

    inter_copy = pltpu.make_async_copy(inter_hbm, inter_ref, inter_sem)
    inter_copy.start()
    index_copy = pltpu.make_async_copy(index_hbm, index_ref, index_sem)
    index_copy.start()
    tile_copy = pltpu.make_async_copy(source_hbm, tile, tile_sem)
    tile_copy.start()
    inter_copy.wait()
    index_copy.wait()
    slots = []
    for place in range(count):
        group = lax.rem(me + place - depth + groups, groups)
        cells_wanted = jnp.zeros((1, index_ref.shape[1]), jnp.int32)
        slot = jnp.int32(0)
        for k in range(count):
            hit = (inter_ref[k] == group).astype(jnp.int32)
            cells_wanted = cells_wanted + index_ref[k : k + 1, :] * hit
            slot = jnp.where(inter_ref[k] == group, jnp.int32(k), slot)
        slots.append(slot)
        if place == depth:
            wanted[place] = cells_wanted
        else:
            request[place] = cells_wanted

    tile_copy.wait()
    weight_copies = []
    for part in range(levs):
        copy = pltpu.make_async_copy(
            blocks_hbm.at[:, :, pl.ds(part * columns, columns)], weights.at[:, part], weight_sem.at[part]
        )
        copy.start()
        weight_copies.append(copy)
    for field in range(fields):
        stack32[pl.ds(field * slab_levels, slab_levels), :] = tile[field].astype(jnp.float32)
    spare = rows - fields * slab_levels
    if spare:
        stack32[pl.ds(fields * slab_levels, spare), :] = jnp.zeros((spare, cells), jnp.float32)
    stack[...] = stack32[...].astype(jnp.bfloat16)

    pl.semaphore_wait(barrier, len(offsets) + levs - 1)

    def request_copy(place):
        return pltpu.make_async_remote_copy(
            src_ref=request.at[place],
            dst_ref=wanted.at[2 * depth - place],
            send_sem=req_send.at[place],
            recv_sem=req_recv.at[2 * depth - place],
            device_id={"horiz": lax.rem(me + place - depth + groups, groups)},
            device_id_type=MESH,
        )

    def value_copy(place):
        return pltpu.make_async_remote_copy(
            src_ref=chosen.at[place],
            dst_ref=arrived.at[2 * depth - place],
            send_sem=val_send.at[place],
            recv_sem=val_recv.at[2 * depth - place],
            device_id={"horiz": lax.rem(me + place - depth + groups, groups)},
            device_id_type=MESH,
        )

    for reach in range(depth, 0, -1):
        request_copy(depth - reach).start()
        request_copy(depth + reach).start()

    ids = lax.broadcasted_iota(jnp.int32, (HIGH, 1), 0).astype(jnp.float32).astype(jnp.bfloat16)

    def select(place):
        cell = wanted[place]
        high = cell // HIGH
        low = (cell - high * HIGH).astype(jnp.float32)
        values = jnp.zeros((rows, cell.shape[1]), jnp.float32)
        for chunk in range(cells // HIGH):
            here = jnp.where(high == chunk, low, -1.0).astype(jnp.bfloat16)
            picker = jnp.where(ids == here, jnp.bfloat16(1), jnp.bfloat16(0))
            values += jnp.dot(
                stack[:, chunk * HIGH : (chunk + 1) * HIGH], picker, preferred_element_type=jnp.float32
            )
        return values.astype(jnp.bfloat16)

    arrived[depth] = select(depth)

    def serve(step, carry):
        reach = depth - step // 2
        place = depth + reach * (1 - 2 * (step % 2))
        request_copy(2 * depth - place).wait_recv()
        chosen[place] = select(place)
        value_copy(place).start()
        return carry

    lax.fori_loop(0, 2 * depth, serve, 0)

    for copy in weight_copies:
        copy.wait()
    order = [depth]
    for reach in range(depth, 0, -1):
        order += [depth - reach, depth + reach]
    for number, place in enumerate(order):
        if number:
            value_copy(2 * depth - place).wait_recv()
        values = arrived[place]
        for hop in list(range(1, levs)) + [0]:
            part = lax.rem(my_lev + hop, levs)
            term = jnp.dot(values, weights[slots[place], part], preferred_element_type=jnp.float32)
            if number == 0:
                total[part] = term
            elif number < count - 1:
                total[part] += term
            else:
                done = (total[part] + term).astype(jnp.bfloat16)
                if hop == 0:
                    out_ref[my_lev] = done
                else:
                    slab[hop] = done
                    lev_copy(hop, part, my_lev, slab, out_ref, lev_send, lev_recv).start()
    for hop in range(1, levs):
        lev_copy(hop, lax.rem(my_lev + hop, levs), my_lev, slab, out_ref, lev_send, lev_recv).wait()
    for offset in offsets:
        request_copy(depth + offset).wait_send()
        value_copy(depth + offset).wait_send()


def lev_copy(hop, part, my_lev, slab, out_ref, lev_send, lev_recv):
    return pltpu.make_async_remote_copy(
        src_ref=slab.at[hop],
        dst_ref=out_ref.at[my_lev],
        send_sem=lev_send.at[hop],
        recv_sem=lev_recv.at[hop],
        device_id={"lev": part},
        device_id_type=MESH,
    )


def rows_at(table, index):
    numbers = lax.GatherDimensionNumbers(
        offset_dims=(),
        collapsed_slice_dims=(0,),
        start_index_map=(0,),
        operand_batching_dims=(1,),
        start_indices_batching_dims=(1,),
    )
    return lax.gather(
        table, index[..., None], numbers, slice_sizes=(1, 1), mode=lax.GatherScatterMode.PROMISE_IN_BOUNDS
    )


def levels_kernel(slab_levels, slabs_ref, bracket_ref, fraction_ref, out_hbm, raw, table, mixed_ref, out_sem):
    levs = slabs_ref.shape[0]
    strips, fields, levels_out, lanes = mixed_ref.shape
    total = levs * slab_levels
    step = 16

    def strip_copy(strip):
        return pltpu.make_async_copy(
            mixed_ref.at[strip],
            out_hbm.at[:, :, pl.ds(pl.multiple_of(strip * lanes, lanes), lanes)],
            out_sem.at[strip],
        )

    def work(strip, carry):
        here_lanes = pl.ds(pl.multiple_of(strip * lanes, lanes), lanes)
        raw[...] = slabs_ref[:, :, here_lanes].astype(jnp.float32)
        for field in range(fields):
            for lev in range(levs):
                table[field, pl.ds(lev * slab_levels, slab_levels), :] = raw[
                    lev, pl.ds(field * slab_levels, slab_levels), :
                ]
        for start in range(0, levels_out, step):
            size = min(step, levels_out - start)
            bracket = bracket_ref[start : start + size, here_lanes]
            upper = fraction_ref[start : start + size, here_lanes]
            if size < step:
                bracket = jnp.concatenate([bracket, jnp.zeros((step - size, lanes), jnp.int32)], axis=0)
                upper = jnp.concatenate([upper, jnp.zeros((step - size, lanes), jnp.float32)], axis=0)
            halves = [bracket[i : i + 8] for i in range(0, step, 8)]
            high = [half >> 3 for half in halves]
            low = [half & 7 for half in halves]
            below = [[jnp.zeros((8, lanes), jnp.float32) for _ in halves] for _ in range(fields)]
            above = [[jnp.zeros((8, lanes), jnp.float32) for _ in halves] for _ in range(fields)]
            for group in range((total - 2) // 8 + 1):
                masks = [h == group for h in high]
                for field in range(fields):
                    here = table[field, pl.ds(group * 8, 8), :]
                    over = table[field, pl.ds(group * 8 + 1, 8), :]
                    for i, mask in enumerate(masks):
                        below[field][i] = jnp.where(mask, rows_at(here, low[i]), below[field][i])
                        above[field][i] = jnp.where(mask, rows_at(over, low[i]), above[field][i])
            for field in range(fields):
                mixed = (1.0 - upper) * jnp.concatenate(below[field], axis=0) + upper * jnp.concatenate(
                    above[field], axis=0
                )
                mixed_ref[strip, field, start : start + size, :] = mixed[:size].astype(jnp.bfloat16)
        strip_copy(strip).start()
        return carry

    for field in range(fields):
        table[field, pl.ds(total, table.shape[1] - total), :] = jnp.zeros(
            (table.shape[1] - total, lanes), jnp.float32
        )
    lax.fori_loop(0, strips, work, 0)
    for strip in range(strips):
        strip_copy(strip).wait()


def local(levs, groups, source_state, intersection, index_map, blocks, bracket, fraction):
    fields, slab_levels, cells = source_state.shape
    count, wide, targets = blocks.shape
    depth = (count - 1) // 2
    rows = round_up(fields * slab_levels, 8)
    columns = targets // levs
    slabs = pl.pallas_call(
        functools.partial(remap_kernel, groups, levs, depth),
        name="remap",
        out_shape=jax.ShapeDtypeStruct((levs, rows, columns), jnp.bfloat16),
        in_specs=[
            pl.BlockSpec(memory_space=pltpu.HBM),
            pl.BlockSpec(memory_space=pltpu.HBM),
            pl.BlockSpec(memory_space=pltpu.HBM),
            pl.BlockSpec(memory_space=pltpu.HBM),
        ],
        out_specs=pl.BlockSpec(memory_space=pltpu.VMEM),
        scratch_shapes=[
            pltpu.SMEM((count,), jnp.int32),
            pltpu.VMEM((count, wide), jnp.int32),
            pltpu.VMEM((fields, slab_levels, cells), jnp.bfloat16),
            pltpu.VMEM((rows, cells), jnp.float32),
            pltpu.VMEM((rows, cells), jnp.bfloat16),
            pltpu.VMEM((count, levs, wide, columns), jnp.bfloat16),
            pltpu.VMEM((count, 1, wide), jnp.int32),
            pltpu.VMEM((count, 1, wide), jnp.int32),
            pltpu.VMEM((count, rows, wide), jnp.bfloat16),
            pltpu.VMEM((count, rows, wide), jnp.bfloat16),
            pltpu.VMEM((levs, rows, columns), jnp.float32),
            pltpu.VMEM((levs, rows, columns), jnp.bfloat16),
            pltpu.SemaphoreType.DMA,
            pltpu.SemaphoreType.DMA,
            pltpu.SemaphoreType.DMA,
            pltpu.SemaphoreType.DMA((levs,)),
            pltpu.SemaphoreType.DMA((count,)),
            pltpu.SemaphoreType.DMA((count,)),
            pltpu.SemaphoreType.DMA((count,)),
            pltpu.SemaphoreType.DMA((count,)),
            pltpu.SemaphoreType.DMA((levs,)),
            pltpu.SemaphoreType.DMA((levs,)),
        ],
        compiler_params=pltpu.CompilerParams(
            collective_id=0, has_side_effects=True, vmem_limit_bytes=67043328 - 1300 * 1024
        ),
        cost_estimate=pl.CostEstimate(
            flops=2 * rows * count * wide * (cells + targets),
            bytes_accessed=2 * blocks.size + 2 * source_state.size,
            transcendentals=0,
        ),
    )(intersection, index_map, source_state, blocks)
    levels_out, held = bracket.shape
    lanes = 128
    return pl.pallas_call(
        functools.partial(levels_kernel, slab_levels),
        name="levels",
        out_shape=jax.ShapeDtypeStruct((fields, levels_out, held), jnp.bfloat16),
        in_specs=[pl.BlockSpec(memory_space=pltpu.VMEM)] * 3,
        out_specs=pl.BlockSpec(memory_space=pltpu.HBM),
        scratch_shapes=[
            pltpu.VMEM((levs, rows, lanes), jnp.float32),
            pltpu.VMEM((fields, round_up(levs * slab_levels, 8) + 8, lanes), jnp.float32),
            pltpu.VMEM((held // lanes, fields, levels_out, lanes), jnp.bfloat16),
            pltpu.SemaphoreType.DMA((held // lanes,)),
        ],
        compiler_params=pltpu.CompilerParams(vmem_limit_bytes=8 * 1024 * 1024),
    )(slabs, bracket, fraction)


def solution(mesh):
    in_specs = (
        P(None, "lev", "horiz"),
        P("horiz"),
        P("horiz", None),
        P("horiz", None, None),
        P(None, ("horiz", "lev")),
        P(None, ("horiz", "lev")),
    )
    out_specs = P(None, None, ("horiz", "lev"))
    body = functools.partial(local, mesh.shape["lev"], mesh.shape["horiz"])
    return jax.shard_map(body, mesh=mesh, in_specs=in_specs, out_specs=out_specs, check_vma=False)
```

```python
import functools

import jax
import jax.numpy as jnp
from jax import lax
from jax.experimental import pallas as pl
from jax.experimental.pallas import tpu as pltpu
from jax.sharding import PartitionSpec as P

MESH = pl.DeviceIdType.MESH
HIGH = 256


def round_up(value, step):
    return (value + step - 1) // step * step


def remap_kernel(
    groups, levs, depth,
    inter_hbm, index_hbm, source_hbm, blocks_hbm, out_ref,
    inter_ref, index_ref, tile, stack32, stack, weights, request, wanted, chosen, arrived, total, slab,
    inter_sem, index_sem, tile_sem, weight_sem, req_send, req_recv, val_send, val_recv, lev_send, lev_recv, own_sem,
):
    fields, slab_levels, cells = tile.shape
    rows = stack.shape[0]
    count = 2 * depth + 1
    me = lax.axis_index("horiz")
    my_lev = lax.axis_index("lev")
    columns = out_ref.shape[2]
    half = round_up(rows // 2, 16)
    cuts = [(0, half), (half, rows - half)]

    barrier = pltpu.get_barrier_semaphore()
    offsets = [o for o in range(-depth, depth + 1) if o != 0]
    for offset in offsets:
        pl.semaphore_signal(
            barrier, inc=1, device_id={"horiz": lax.rem(me + offset + groups, groups)}, device_id_type=MESH
        )
    for hop in range(1, levs):
        pl.semaphore_signal(
            barrier, inc=1, device_id={"lev": lax.rem(my_lev + hop, levs)}, device_id_type=MESH
        )

    inter_copy = pltpu.make_async_copy(inter_hbm, inter_ref, inter_sem)
    inter_copy.start()
    index_copy = pltpu.make_async_copy(index_hbm, index_ref, index_sem)
    index_copy.start()
    tile_copy = pltpu.make_async_copy(source_hbm, tile, tile_sem)
    tile_copy.start()
    inter_copy.wait()
    index_copy.wait()
    slots = []
    for place in range(count):
        group = lax.rem(me + place - depth + groups, groups)
        cells_wanted = jnp.zeros((1, index_ref.shape[1]), jnp.int32)
        slot = jnp.int32(0)
        for k in range(count):
            hit = (inter_ref[k] == group).astype(jnp.int32)
            cells_wanted = cells_wanted + index_ref[k : k + 1, :] * hit
            slot = jnp.where(inter_ref[k] == group, jnp.int32(k), slot)
        slots.append(slot)
        if place == depth:
            wanted[place] = cells_wanted
        else:
            request[place] = cells_wanted

    tile_copy.wait()
    weight_copies = []
    for part in range(levs):
        copy = pltpu.make_async_copy(
            blocks_hbm.at[:, :, pl.ds(part * columns, columns)], weights.at[:, part], weight_sem.at[part]
        )
        copy.start()
        weight_copies.append(copy)
    for field in range(fields):
        stack32[pl.ds(field * slab_levels, slab_levels), :] = tile[field].astype(jnp.float32)
    spare = rows - fields * slab_levels
    if spare:
        stack32[pl.ds(fields * slab_levels, spare), :] = jnp.zeros((spare, cells), jnp.float32)
    stack[...] = stack32[...].astype(jnp.bfloat16)

    pl.semaphore_wait(barrier, len(offsets) + levs - 1)

    def request_copy(place):
        return pltpu.make_async_remote_copy(
            src_ref=request.at[place],
            dst_ref=wanted.at[2 * depth - place],
            send_sem=req_send.at[place],
            recv_sem=req_recv.at[2 * depth - place],
            device_id={"horiz": lax.rem(me + place - depth + groups, groups)},
            device_id_type=MESH,
        )

    def value_copy(place, piece):
        first, size = cuts[piece]
        return pltpu.make_async_remote_copy(
            src_ref=chosen.at[place, pl.ds(first, size)],
            dst_ref=arrived.at[2 * depth - place, pl.ds(first, size)],
            send_sem=val_send.at[piece, place],
            recv_sem=val_recv.at[piece, 2 * depth - place],
            device_id={"horiz": lax.rem(me + place - depth + groups, groups)},
            device_id_type=MESH,
        )

    def lev_copy(hop, piece):
        block = pl.ds(*cuts[piece])
        if hop == 0:
            return pltpu.make_async_copy(slab.at[0, block], out_ref.at[my_lev, block], own_sem.at[piece])
        return pltpu.make_async_remote_copy(
            src_ref=slab.at[hop, block],
            dst_ref=out_ref.at[my_lev, block],
            send_sem=lev_send.at[piece, hop],
            recv_sem=lev_recv.at[piece, hop],
            device_id={"lev": lax.rem(my_lev + hop, levs)},
            device_id_type=MESH,
        )

    for reach in range(depth, 0, -1):
        request_copy(depth - reach).start()
        request_copy(depth + reach).start()

    ids = lax.broadcasted_iota(jnp.int32, (HIGH, 1), 0).astype(jnp.float32).astype(jnp.bfloat16)

    def select(place):
        cell = wanted[place]
        high = cell // HIGH
        low = (cell - high * HIGH).astype(jnp.float32)
        values = jnp.zeros((rows, cell.shape[1]), jnp.float32)
        for chunk in range(cells // HIGH):
            here = jnp.where(high == chunk, low, -1.0).astype(jnp.bfloat16)
            picker = jnp.where(ids == here, jnp.bfloat16(1), jnp.bfloat16(0))
            values += jnp.dot(
                stack[:, chunk * HIGH : (chunk + 1) * HIGH], picker, preferred_element_type=jnp.float32
            )
        return values.astype(jnp.bfloat16)

    arrived[depth] = select(depth)

    def serve(step, carry):
        reach = depth - step // 2
        place = depth + reach * (1 - 2 * (step % 2))
        request_copy(2 * depth - place).wait_recv()
        chosen[place] = select(place)
        value_copy(place, 0).start()
        return carry

    lax.fori_loop(0, 2 * depth, serve, 0)

    for reach in range(depth, 0, -1):
        value_copy(depth - reach, 1).start()
        value_copy(depth + reach, 1).start()
    for copy in weight_copies:
        copy.wait()
    order = [depth]
    for reach in range(depth, 0, -1):
        order += [depth - reach, depth + reach]
    for piece, (first, size) in enumerate(cuts):
        block = pl.ds(first, size)
        for number, place in enumerate(order):
            if number:
                value_copy(2 * depth - place, piece).wait_recv()
            values = arrived[place, block]
            for hop in list(range(1, levs)) + [0]:
                part = lax.rem(my_lev + hop, levs)
                term = jnp.dot(values, weights[slots[place], part], preferred_element_type=jnp.float32)
                if number == 0:
                    total[part, block] = term
                elif number < count - 1:
                    total[part, block] += term
                else:
                    slab[hop, block] = (total[part, block] + term).astype(jnp.bfloat16)
                    lev_copy(hop, piece).start()
    for piece in range(len(cuts)):
        for hop in range(levs):
            lev_copy(hop, piece).wait()
        for offset in offsets:
            value_copy(depth + offset, piece).wait_send()
    for offset in offsets:
        request_copy(depth + offset).wait_send()


def rows_at(table, index):
    numbers = lax.GatherDimensionNumbers(
        offset_dims=(),
        collapsed_slice_dims=(0,),
        start_index_map=(0,),
        operand_batching_dims=(1,),
        start_indices_batching_dims=(1,),
    )
    return lax.gather(
        table, index[..., None], numbers, slice_sizes=(1, 1), mode=lax.GatherScatterMode.PROMISE_IN_BOUNDS
    )


def levels_kernel(
    slab_levels, slabs_hbm, bracket_ref, fraction_ref, out_hbm, slabs_ref, raw, table, mixed_ref, slab_sem, out_sem
):
    levs = slabs_hbm.shape[0]
    strips, fields, levels_out, lanes = mixed_ref.shape
    total = levs * slab_levels
    step = 16

    def strip_copy(strip):
        return pltpu.make_async_copy(
            mixed_ref.at[strip],
            out_hbm.at[:, :, pl.ds(pl.multiple_of(strip * lanes, lanes), lanes)],
            out_sem.at[strip],
        )

    def slab_copy(strip):
        return pltpu.make_async_copy(
            slabs_hbm.at[:, :, pl.ds(pl.multiple_of(strip * lanes, lanes), lanes)],
            slabs_ref.at[strip],
            slab_sem.at[strip],
        )

    for strip in range(strips):
        slab_copy(strip).start()

    def work(strip, carry):
        here_lanes = pl.ds(pl.multiple_of(strip * lanes, lanes), lanes)
        slab_copy(strip).wait()
        raw[...] = slabs_ref[strip].astype(jnp.float32)
        for field in range(fields):
            for lev in range(levs):
                table[field, pl.ds(lev * slab_levels, slab_levels), :] = raw[
                    lev, pl.ds(field * slab_levels, slab_levels), :
                ]
        for start in range(0, levels_out, step):
            size = min(step, levels_out - start)
            bracket = bracket_ref[start : start + size, here_lanes]
            upper = fraction_ref[start : start + size, here_lanes]
            if size < step:
                bracket = jnp.concatenate([bracket, jnp.zeros((step - size, lanes), jnp.int32)], axis=0)
                upper = jnp.concatenate([upper, jnp.zeros((step - size, lanes), jnp.float32)], axis=0)
            halves = [bracket[i : i + 8] for i in range(0, step, 8)]
            high = [half >> 3 for half in halves]
            low = [half & 7 for half in halves]
            below = [[jnp.zeros((8, lanes), jnp.float32) for _ in halves] for _ in range(fields)]
            above = [[jnp.zeros((8, lanes), jnp.float32) for _ in halves] for _ in range(fields)]
            for group in range((total - 2) // 8 + 1):
                masks = [h == group for h in high]
                for field in range(fields):
                    here = table[field, pl.ds(group * 8, 8), :]
                    over = table[field, pl.ds(group * 8 + 1, 8), :]
                    for i, mask in enumerate(masks):
                        below[field][i] = jnp.where(mask, rows_at(here, low[i]), below[field][i])
                        above[field][i] = jnp.where(mask, rows_at(over, low[i]), above[field][i])
            for field in range(fields):
                mixed = (1.0 - upper) * jnp.concatenate(below[field], axis=0) + upper * jnp.concatenate(
                    above[field], axis=0
                )
                mixed_ref[strip, field, start : start + size, :] = mixed[:size].astype(jnp.bfloat16)
        strip_copy(strip).start()
        return carry

    for field in range(fields):
        table[field, pl.ds(total, table.shape[1] - total), :] = jnp.zeros(
            (table.shape[1] - total, lanes), jnp.float32
        )
    lax.fori_loop(0, strips, work, 0)
    for strip in range(strips):
        strip_copy(strip).wait()


def local(levs, groups, source_state, intersection, index_map, blocks, bracket, fraction):
    fields, slab_levels, cells = source_state.shape
    count, wide, targets = blocks.shape
    depth = (count - 1) // 2
    rows = round_up(fields * slab_levels, 8)
    columns = targets // levs
    slabs = pl.pallas_call(
        functools.partial(remap_kernel, groups, levs, depth),
        name="remap",
        out_shape=jax.ShapeDtypeStruct((levs, rows, columns), jnp.bfloat16),
        in_specs=[
            pl.BlockSpec(memory_space=pltpu.HBM),
            pl.BlockSpec(memory_space=pltpu.HBM),
            pl.BlockSpec(memory_space=pltpu.HBM),
            pl.BlockSpec(memory_space=pltpu.HBM),
        ],
        out_specs=pl.BlockSpec(memory_space=pltpu.HBM),
        scratch_shapes=[
            pltpu.SMEM((count,), jnp.int32),
            pltpu.VMEM((count, wide), jnp.int32),
            pltpu.VMEM((fields, slab_levels, cells), jnp.bfloat16),
            pltpu.VMEM((rows, cells), jnp.float32),
            pltpu.VMEM((rows, cells), jnp.bfloat16),
            pltpu.VMEM((count, levs, wide, columns), jnp.bfloat16),
            pltpu.VMEM((count, 1, wide), jnp.int32),
            pltpu.VMEM((count, 1, wide), jnp.int32),
            pltpu.VMEM((count, rows, wide), jnp.bfloat16),
            pltpu.VMEM((count, rows, wide), jnp.bfloat16),
            pltpu.VMEM((levs, rows, columns), jnp.float32),
            pltpu.VMEM((levs, rows, columns), jnp.bfloat16),
            pltpu.SemaphoreType.DMA,
            pltpu.SemaphoreType.DMA,
            pltpu.SemaphoreType.DMA,
            pltpu.SemaphoreType.DMA((levs,)),
            pltpu.SemaphoreType.DMA((count,)),
            pltpu.SemaphoreType.DMA((count,)),
            pltpu.SemaphoreType.DMA((2, count)),
            pltpu.SemaphoreType.DMA((2, count)),
            pltpu.SemaphoreType.DMA((2, levs)),
            pltpu.SemaphoreType.DMA((2, levs)),
            pltpu.SemaphoreType.DMA((2,)),
        ],
        compiler_params=pltpu.CompilerParams(
            collective_id=0, has_side_effects=True, vmem_limit_bytes=67043328 - 1300 * 1024
        ),
        cost_estimate=pl.CostEstimate(
            flops=2 * rows * count * wide * (cells + targets),
            bytes_accessed=2 * blocks.size + 2 * source_state.size,
            transcendentals=0,
        ),
    )(intersection, index_map, source_state, blocks)
    levels_out, held = bracket.shape
    lanes = 128
    return pl.pallas_call(
        functools.partial(levels_kernel, slab_levels),
        name="levels",
        out_shape=jax.ShapeDtypeStruct((fields, levels_out, held), jnp.bfloat16),
        in_specs=[
            pl.BlockSpec(memory_space=pltpu.HBM),
            pl.BlockSpec(memory_space=pltpu.VMEM),
            pl.BlockSpec(memory_space=pltpu.VMEM),
        ],
        out_specs=pl.BlockSpec(memory_space=pltpu.HBM),
        scratch_shapes=[
            pltpu.VMEM((held // lanes, levs, rows, lanes), jnp.bfloat16),
            pltpu.VMEM((levs, rows, lanes), jnp.float32),
            pltpu.VMEM((fields, round_up(levs * slab_levels, 8) + 8, lanes), jnp.float32),
            pltpu.VMEM((held // lanes, fields, levels_out, lanes), jnp.bfloat16),
            pltpu.SemaphoreType.DMA((held // lanes,)),
            pltpu.SemaphoreType.DMA((held // lanes,)),
        ],
        compiler_params=pltpu.CompilerParams(vmem_limit_bytes=67043328 - 700 * 1024),
    )(slabs, bracket, fraction)


def solution(mesh):
    in_specs = (
        P(None, "lev", "horiz"),
        P("horiz"),
        P("horiz", None),
        P("horiz", None, None),
        P(None, ("horiz", "lev")),
        P(None, ("horiz", "lev")),
    )
    out_specs = P(None, None, ("horiz", "lev"))
    body = functools.partial(local, mesh.shape["lev"], mesh.shape["horiz"])
    return jax.shard_map(body, mesh=mesh, in_specs=in_specs, out_specs=out_specs, check_vma=False)
```

```python
import functools

import jax
import jax.numpy as jnp
from jax import lax
from jax.experimental import pallas as pl
from jax.experimental.pallas import tpu as pltpu
from jax.sharding import PartitionSpec as P

MESH = pl.DeviceIdType.MESH
HIGH = 256


def round_up(value, step):
    return (value + step - 1) // step * step


def remap_kernel(
    groups, levs, depth,
    inter_hbm, index_hbm, source_hbm, blocks_hbm, out_ref,
    inter_ref, index_ref, tile, stack32, stack, weights, request, wanted, chosen, arrived, total, slab,
    inter_sem, index_sem, tile_sem, weight_sem, req_send, req_recv, val_send, val_recv, lev_send, lev_recv, own_sem,
):
    fields, slab_levels, cells = tile.shape
    rows = stack.shape[0]
    count = 2 * depth + 1
    me = lax.axis_index("horiz")
    my_lev = lax.axis_index("lev")
    columns = out_ref.shape[2]
    half = round_up(rows // 2, 16)
    cuts = [(0, half), (half, rows - half)]

    barrier = pltpu.get_barrier_semaphore()
    offsets = [o for o in range(-depth, depth + 1) if o != 0]
    for offset in offsets:
        pl.semaphore_signal(
            barrier, inc=1, device_id={"horiz": lax.rem(me + offset + groups, groups)}, device_id_type=MESH
        )
    for hop in range(1, levs):
        pl.semaphore_signal(
            barrier, inc=1, device_id={"lev": lax.rem(my_lev + hop, levs)}, device_id_type=MESH
        )

    inter_copy = pltpu.make_async_copy(inter_hbm, inter_ref, inter_sem)
    inter_copy.start()
    index_copy = pltpu.make_async_copy(index_hbm, index_ref, index_sem)
    index_copy.start()
    tile_copy = pltpu.make_async_copy(source_hbm, tile, tile_sem)
    tile_copy.start()
    inter_copy.wait()
    index_copy.wait()
    slots = []
    for place in range(count):
        group = lax.rem(me + place - depth + groups, groups)
        cells_wanted = jnp.zeros((1, index_ref.shape[1]), jnp.int32)
        slot = jnp.int32(0)
        for k in range(count):
            hit = (inter_ref[k] == group).astype(jnp.int32)
            cells_wanted = cells_wanted + index_ref[k : k + 1, :] * hit
            slot = jnp.where(inter_ref[k] == group, jnp.int32(k), slot)
        slots.append(slot)
        if place == depth:
            wanted[place] = cells_wanted
        else:
            request[place] = cells_wanted

    tile_copy.wait()
    weight_copies = []
    for part in range(levs):
        copy = pltpu.make_async_copy(
            blocks_hbm.at[:, :, pl.ds(part * columns, columns)], weights.at[:, part], weight_sem.at[part]
        )
        copy.start()
        weight_copies.append(copy)
    for field in range(fields):
        stack32[pl.ds(field * slab_levels, slab_levels), :] = tile[field].astype(jnp.float32)
    spare = rows - fields * slab_levels
    if spare:
        stack32[pl.ds(fields * slab_levels, spare), :] = jnp.zeros((spare, cells), jnp.float32)
    stack[...] = stack32[...].astype(jnp.bfloat16)

    pl.semaphore_wait(barrier, len(offsets) + levs - 1)

    def request_copy(place):
        return pltpu.make_async_remote_copy(
            src_ref=request.at[place],
            dst_ref=wanted.at[2 * depth - place],
            send_sem=req_send.at[place],
            recv_sem=req_recv.at[2 * depth - place],
            device_id={"horiz": lax.rem(me + place - depth + groups, groups)},
            device_id_type=MESH,
        )

    def value_copy(place, piece):
        first, size = cuts[piece]
        return pltpu.make_async_remote_copy(
            src_ref=chosen.at[place, pl.ds(first, size)],
            dst_ref=arrived.at[2 * depth - place, pl.ds(first, size)],
            send_sem=val_send.at[piece, place],
            recv_sem=val_recv.at[piece, 2 * depth - place],
            device_id={"horiz": lax.rem(me + place - depth + groups, groups)},
            device_id_type=MESH,
        )

    def lev_copy(hop, piece):
        block = pl.ds(*cuts[piece])
        if hop == 0:
            return pltpu.make_async_copy(slab.at[0, block], out_ref.at[my_lev, block], own_sem.at[piece])
        return pltpu.make_async_remote_copy(
            src_ref=slab.at[hop, block],
            dst_ref=out_ref.at[my_lev, block],
            send_sem=lev_send.at[piece, hop],
            recv_sem=lev_recv.at[piece, hop],
            device_id={"lev": lax.rem(my_lev + hop, levs)},
            device_id_type=MESH,
        )

    for reach in range(depth, 0, -1):
        request_copy(depth - reach).start()
        request_copy(depth + reach).start()

    ids = lax.broadcasted_iota(jnp.int32, (HIGH, 1), 0).astype(jnp.float32).astype(jnp.bfloat16)

    def select(place):
        cell = wanted[place]
        high = cell // HIGH
        low = (cell - high * HIGH).astype(jnp.float32)
        values = jnp.zeros((rows, cell.shape[1]), jnp.float32)
        for chunk in range(cells // HIGH):
            here = jnp.where(high == chunk, low, -1.0).astype(jnp.bfloat16)
            picker = jnp.where(ids == here, jnp.bfloat16(1), jnp.bfloat16(0))
            values += jnp.dot(
                stack[:, chunk * HIGH : (chunk + 1) * HIGH], picker, preferred_element_type=jnp.float32
            )
        return values.astype(jnp.bfloat16)

    arrived[depth] = select(depth)

    def serve(step, carry):
        reach = depth - step // 2
        place = depth + reach * (1 - 2 * (step % 2))
        request_copy(2 * depth - place).wait_recv()
        chosen[place] = select(place)
        value_copy(place, 0).start()
        return carry

    lax.fori_loop(0, 2 * depth, serve, 0)

    for reach in range(depth, 0, -1):
        value_copy(depth - reach, 1).start()
        value_copy(depth + reach, 1).start()
    for copy in weight_copies:
        copy.wait()
    order = [depth]
    for reach in range(depth, 0, -1):
        order += [depth - reach, depth + reach]
    for piece, (first, size) in enumerate(cuts):
        block = pl.ds(first, size)
        for number, place in enumerate(order):
            if number:
                value_copy(2 * depth - place, piece).wait_recv()
            values = arrived[place, block]
            for hop in list(range(1, levs)) + [0]:
                part = lax.rem(my_lev + hop, levs)
                term = jnp.dot(values, weights[slots[place], part], preferred_element_type=jnp.float32)
                if number == 0:
                    total[part, block] = term
                elif number < count - 1:
                    total[part, block] += term
                else:
                    slab[hop, block] = (total[part, block] + term).astype(jnp.bfloat16)
                    lev_copy(hop, piece).start()
    for piece in range(len(cuts)):
        for hop in range(levs):
            lev_copy(hop, piece).wait()
        for offset in offsets:
            value_copy(depth + offset, piece).wait_send()
    for offset in offsets:
        request_copy(depth + offset).wait_send()


def rows_at(table, index):
    numbers = lax.GatherDimensionNumbers(
        offset_dims=(),
        collapsed_slice_dims=(0,),
        start_index_map=(0,),
        operand_batching_dims=(1,),
        start_indices_batching_dims=(1,),
    )
    return lax.gather(
        table, index[..., None], numbers, slice_sizes=(1, 1), mode=lax.GatherScatterMode.PROMISE_IN_BOUNDS
    )


def levels_kernel(
    slab_levels, slabs_hbm, bracket_hbm, fraction_hbm, out_hbm,
    slabs_ref, brackets, fractions, raw, table, mixed_ref, slab_sem, bracket_sem, fraction_sem, out_sem,
):
    levs = slabs_hbm.shape[0]
    strips, fields, levels_out, lanes = mixed_ref.shape
    total = levs * slab_levels
    step = 16

    def strip_copy(strip):
        return pltpu.make_async_copy(
            mixed_ref.at[strip],
            out_hbm.at[:, :, pl.ds(pl.multiple_of(strip * lanes, lanes), lanes)],
            out_sem.at[strip],
        )

    def slab_copy(strip):
        return pltpu.make_async_copy(
            slabs_hbm.at[:, :, pl.ds(pl.multiple_of(strip * lanes, lanes), lanes)],
            slabs_ref.at[strip],
            slab_sem.at[strip],
        )

    def bracket_copy(strip):
        return pltpu.make_async_copy(
            bracket_hbm.at[:, pl.ds(pl.multiple_of(strip * lanes, lanes), lanes)],
            brackets.at[strip],
            bracket_sem.at[strip],
        )

    def fraction_copy(strip):
        return pltpu.make_async_copy(
            fraction_hbm.at[:, pl.ds(pl.multiple_of(strip * lanes, lanes), lanes)],
            fractions.at[strip],
            fraction_sem.at[strip],
        )

    for strip in range(strips):
        slab_copy(strip).start()
        bracket_copy(strip).start()
        fraction_copy(strip).start()

    def work(strip, carry):
        slab_copy(strip).wait()
        bracket_copy(strip).wait()
        fraction_copy(strip).wait()
        raw[...] = slabs_ref[strip].astype(jnp.float32)
        for field in range(fields):
            for lev in range(levs):
                table[field, pl.ds(lev * slab_levels, slab_levels), :] = raw[
                    lev, pl.ds(field * slab_levels, slab_levels), :
                ]
        for start in range(0, levels_out, step):
            size = min(step, levels_out - start)
            bracket = brackets[strip, start : start + size, :]
            upper = fractions[strip, start : start + size, :]
            if size < step:
                bracket = jnp.concatenate([bracket, jnp.zeros((step - size, lanes), jnp.int32)], axis=0)
                upper = jnp.concatenate([upper, jnp.zeros((step - size, lanes), jnp.float32)], axis=0)
            halves = [bracket[i : i + 8] for i in range(0, step, 8)]
            high = [half >> 3 for half in halves]
            low = [half & 7 for half in halves]
            below = [[jnp.zeros((8, lanes), jnp.float32) for _ in halves] for _ in range(fields)]
            above = [[jnp.zeros((8, lanes), jnp.float32) for _ in halves] for _ in range(fields)]
            for group in range((total - 2) // 8 + 1):
                masks = [h == group for h in high]
                for field in range(fields):
                    here = table[field, pl.ds(group * 8, 8), :]
                    over = table[field, pl.ds(group * 8 + 1, 8), :]
                    for i, mask in enumerate(masks):
                        below[field][i] = jnp.where(mask, rows_at(here, low[i]), below[field][i])
                        above[field][i] = jnp.where(mask, rows_at(over, low[i]), above[field][i])
            for field in range(fields):
                mixed = (1.0 - upper) * jnp.concatenate(below[field], axis=0) + upper * jnp.concatenate(
                    above[field], axis=0
                )
                mixed_ref[strip, field, start : start + size, :] = mixed[:size].astype(jnp.bfloat16)
        strip_copy(strip).start()
        return carry

    for field in range(fields):
        table[field, pl.ds(total, table.shape[1] - total), :] = jnp.zeros(
            (table.shape[1] - total, lanes), jnp.float32
        )
    lax.fori_loop(0, strips, work, 0)
    for strip in range(strips):
        strip_copy(strip).wait()


def local(levs, groups, source_state, intersection, index_map, blocks, bracket, fraction):
    fields, slab_levels, cells = source_state.shape
    count, wide, targets = blocks.shape
    depth = (count - 1) // 2
    rows = round_up(fields * slab_levels, 8)
    columns = targets // levs
    slabs = pl.pallas_call(
        functools.partial(remap_kernel, groups, levs, depth),
        name="remap",
        out_shape=jax.ShapeDtypeStruct((levs, rows, columns), jnp.bfloat16),
        in_specs=[
            pl.BlockSpec(memory_space=pltpu.HBM),
            pl.BlockSpec(memory_space=pltpu.HBM),
            pl.BlockSpec(memory_space=pltpu.HBM),
            pl.BlockSpec(memory_space=pltpu.HBM),
        ],
        out_specs=pl.BlockSpec(memory_space=pltpu.HBM),
        scratch_shapes=[
            pltpu.SMEM((count,), jnp.int32),
            pltpu.VMEM((count, wide), jnp.int32),
            pltpu.VMEM((fields, slab_levels, cells), jnp.bfloat16),
            pltpu.VMEM((rows, cells), jnp.float32),
            pltpu.VMEM((rows, cells), jnp.bfloat16),
            pltpu.VMEM((count, levs, wide, columns), jnp.bfloat16),
            pltpu.VMEM((count, 1, wide), jnp.int32),
            pltpu.VMEM((count, 1, wide), jnp.int32),
            pltpu.VMEM((count, rows, wide), jnp.bfloat16),
            pltpu.VMEM((count, rows, wide), jnp.bfloat16),
            pltpu.VMEM((levs, rows, columns), jnp.float32),
            pltpu.VMEM((levs, rows, columns), jnp.bfloat16),
            pltpu.SemaphoreType.DMA,
            pltpu.SemaphoreType.DMA,
            pltpu.SemaphoreType.DMA,
            pltpu.SemaphoreType.DMA((levs,)),
            pltpu.SemaphoreType.DMA((count,)),
            pltpu.SemaphoreType.DMA((count,)),
            pltpu.SemaphoreType.DMA((2, count)),
            pltpu.SemaphoreType.DMA((2, count)),
            pltpu.SemaphoreType.DMA((2, levs)),
            pltpu.SemaphoreType.DMA((2, levs)),
            pltpu.SemaphoreType.DMA((2,)),
        ],
        compiler_params=pltpu.CompilerParams(
            collective_id=0, has_side_effects=True, vmem_limit_bytes=67043328 - 1300 * 1024
        ),
        cost_estimate=pl.CostEstimate(
            flops=2 * rows * count * wide * (cells + targets),
            bytes_accessed=2 * blocks.size + 2 * source_state.size,
            transcendentals=0,
        ),
    )(intersection, index_map, source_state, blocks)
    levels_out, held = bracket.shape
    lanes = 128
    return pl.pallas_call(
        functools.partial(levels_kernel, slab_levels),
        name="levels",
        out_shape=jax.ShapeDtypeStruct((fields, levels_out, held), jnp.bfloat16),
        in_specs=[pl.BlockSpec(memory_space=pltpu.HBM)] * 3,
        out_specs=pl.BlockSpec(memory_space=pltpu.HBM),
        scratch_shapes=[
            pltpu.VMEM((held // lanes, levs, rows, lanes), jnp.bfloat16),
            pltpu.VMEM((held // lanes, levels_out, lanes), jnp.int32),
            pltpu.VMEM((held // lanes, levels_out, lanes), jnp.float32),
            pltpu.VMEM((levs, rows, lanes), jnp.float32),
            pltpu.VMEM((fields, round_up(levs * slab_levels, 8) + 8, lanes), jnp.float32),
            pltpu.VMEM((held // lanes, fields, levels_out, lanes), jnp.bfloat16),
            pltpu.SemaphoreType.DMA((held // lanes,)),
            pltpu.SemaphoreType.DMA((held // lanes,)),
            pltpu.SemaphoreType.DMA((held // lanes,)),
            pltpu.SemaphoreType.DMA((held // lanes,)),
        ],
        compiler_params=pltpu.CompilerParams(vmem_limit_bytes=67043328 - 700 * 1024),
    )(slabs, bracket, fraction)


def solution(mesh):
    in_specs = (
        P(None, "lev", "horiz"),
        P("horiz"),
        P("horiz", None),
        P("horiz", None, None),
        P(None, ("horiz", "lev")),
        P(None, ("horiz", "lev")),
    )
    out_specs = P(None, None, ("horiz", "lev"))
    body = functools.partial(local, mesh.shape["lev"], mesh.shape["horiz"])
    return jax.shard_map(body, mesh=mesh, in_specs=in_specs, out_specs=out_specs, check_vma=False)
```
